32 devices in a mesh: row: 8 (over y, x, core), col: 4 (over z).
Axes of the slice: x: 2, y: 2, z: 4, core: 2. Of those that a mesh axis runs over, the one named last changes fastest.
Arguments:
- residual: bfloat16 [8, 4, 2048, 512], P('row', 'col'), may hold values from -6 to 6
- self_tiles: bfloat16 [8, 4, 2048, 2048], P('row', 'col'), may hold values from -0.09375 to 0.09375
- side_tiles: bfloat16 [8, 4, 2048, 2048], P('row', 'col'), may hold values from -0.09375 to 0.09375
- row_cluster_basis: bfloat16 [8, 4, 2048, 32], P('row', 'col'), may hold values from -0.125 to 0.125
- column_cluster_basis: bfloat16 [8, 4, 2048, 32], P('row', 'col'), may hold values from -1 to 1
- couplings: bfloat16 [8, 4, 64, 32, 32], P('row', 'col'), may hold values from -0.1875 to 0.1875
- near_side: int32 [8, 4], P('row', 'col'), may hold values from -1 to 1
- adm_targets: int32 [8, 4, 64], P('row', 'col'), may hold values from 0 to 31, as said below
- adm_ranks: int32 [8, 4, 64], P('row', 'col'), may hold values from 8 to 32
- adm_count: int32 [8, 4], P('row', 'col'), may hold values from 1 to 64
Outputs:
- gradient: float32 [8, 4, 2048, 512], P('row', 'col')
The draws below stay inside these ranges and needn't reach their ends.
Inputs may be any that keep to these rules, and one draw needn't show every extreme that they name: `near_side`: -1 or +1 names the cluster row before or after around the loop of 8 rows; 0 means no such tile. Each entry of adm_targets for the block row of linear index i is the linear index of a cluster other than i; slot 0 names i - 1 or i + 1, counted round the 32 clusters; targets may repeat.
All inputs are finite; a program needn't handle non-finite values.
Results may differ from the reference program's by a relative error of at most 0.0033.
Values may be sent and summed in bfloat16 or wider, within the bound.
A program may use at most 128 MiB of HBM per device.

```python
import jax
import jax.numpy as jnp
from jax import lax

LEAF = 2048
K = 32
NRHS = 512
ADM = 64
GRID_R = 8
GRID_C = 4


def draw_adm_targets(key, part):
    base = jax.random.fold_in(key, 11)
    first_key, second_key = jax.random.split(base)
    total = GRID_R * GRID_C
    linear = (jnp.arange(GRID_R, dtype=jnp.int32)[:, None] * GRID_C + jnp.arange(GRID_C, dtype=jnp.int32)[None, :])[:, :, None]
    offsets = jax.random.randint(first_key, (GRID_R, GRID_C, ADM), 1, total, dtype=jnp.int32)
    signs = jax.random.randint(second_key, (GRID_R, GRID_C, 1), 0, 2, dtype=jnp.int32) * 2 - 1
    slot_index = jnp.arange(ADM, dtype=jnp.int32)[None, None, :]
    chosen = jnp.where(slot_index == 0, signs + total, offsets)
    return ((linear + chosen) % total).astype(jnp.int32)


def plant(values, key, least, largest):
    shape = values.shape
    index_at = [jax.random.randint(jax.random.fold_in(key, axis), (), 0, shape[axis]) for axis in range(len(shape))]
    values = values.at[tuple(index_at)].set(least)
    longest = shape.index(max(shape))
    index_at[longest] = (index_at[longest] + 1) % shape[longest]
    return values.at[tuple(index_at)].set(largest)


def levels(stream_key, shape, cuts, least, high):
    factor_of = 1.0
    for dim, blocks in cuts:
        heights = jax.random.uniform(jax.random.fold_in(jax.random.fold_in(stream_key, 6), dim), (blocks,), jnp.float32, least / len(cuts), high / len(cuts))
        factor_of = factor_of * jnp.repeat(jnp.exp(heights), shape[dim] // blocks).reshape((-1,) + (1,) * (len(shape) - 1 - dim))
    return factor_of


def centred(stream_key, shape, width, limit, pieces=(), held_as=jnp.bfloat16):
    level = levels(stream_key, shape, pieces, -0.22, 0.18) if pieces else 1.0
    values = jax.random.normal(stream_key, shape, jnp.float32) * width * level
    return jnp.minimum(jnp.maximum(values, -limit), limit).astype(held_as)


def setup_inputs(seed: int = 0) -> dict:
    key_of = jax.random.split(jax.random.key(seed), 11)
    return {
        "residual": centred(key_of[0], (GRID_R, GRID_C, LEAF, NRHS), 1.0, 6.0, ((0, 8), (1, 4))),
        "self_tiles": centred(key_of[1], (GRID_R, GRID_C, LEAF, LEAF), (2 * LEAF) ** -0.5, 0.09375, ((0, 8), (1, 4))),
        "side_tiles": centred(key_of[2], (GRID_R, GRID_C, LEAF, LEAF), (2 * LEAF) ** -0.5, 0.09375, ((0, 8), (1, 4))),
        "row_cluster_basis": centred(key_of[3], (GRID_R, GRID_C, LEAF, K), LEAF ** -0.5, 0.125, ((0, 8), (1, 4))),
        "column_cluster_basis": centred(key_of[4], (GRID_R, GRID_C, LEAF, K), K ** -0.5, 1.0, ((0, 8), (1, 4))),
        "couplings": centred(key_of[5], (GRID_R, GRID_C, ADM, K, K), (K * ADM // 2) ** -0.5, 0.1875, ((0, 8), (1, 4))),
        "near_side": plant(jax.random.randint(key_of[6], (GRID_R, GRID_C), -1, 2), jax.random.fold_in(key_of[6], 1), -1, 1).astype(jnp.int32),
        "adm_targets": draw_adm_targets(jax.random.fold_in(key_of[10], 71), 0),
        "adm_ranks": plant(jax.random.randint(key_of[8], (GRID_R, GRID_C, ADM), K // 4, K + 1), jax.random.fold_in(key_of[8], 1), K // 4, K).astype(jnp.int32),
        "adm_count": plant(jax.random.randint(key_of[9], (GRID_R, GRID_C), 1, ADM + 1), jax.random.fold_in(key_of[9], 1), 1, ADM).astype(jnp.int32),
    }


def reference(residual, self_tiles, side_tiles, row_cluster_basis, column_cluster_basis, couplings, near_side, adm_targets, adm_ranks, adm_count):
    grid_rows, grid_cols, sample_points, columns = residual.shape
    slot_count = couplings.shape[2]
    rank_dimension = couplings.shape[3]
    cluster_groups = grid_rows * grid_cols
    flattened_result = residual.reshape(cluster_groups, sample_points, columns)
    coefficient_table = jnp.einsum("qhs,qhe->qse", row_cluster_basis.reshape(cluster_groups, sample_points, rank_dimension).astype(jnp.float32), flattened_result.astype(jnp.float32), precision=lax.Precision.HIGHEST).astype(jnp.bfloat16)
    rank_index = jnp.arange(rank_dimension, dtype=jnp.int32)
    slot_index = jnp.arange(slot_count, dtype=jnp.int32)
    keep_mask = (rank_index[None, None, None, :] < adm_ranks[:, :, :, None]) & (slot_index[None, None, :, None] < adm_count[:, :, None, None])
    keep_float = keep_mask.astype(jnp.float32)
    masked = couplings.astype(jnp.float32) * keep_float[:, :, :, :, None] * keep_float[:, :, :, None, :]
    masked = masked.reshape(cluster_groups, slot_count, rank_dimension, rank_dimension)
    targets = adm_targets.reshape(cluster_groups, slot_count).astype(jnp.int32)

    def add_row(running, inputs):
        block, coeff_block, target_row = inputs
        contrib = jnp.einsum("sab,an->sbn", block, coeff_block.astype(jnp.float32), precision=lax.Precision.HIGHEST)
        return running.at[target_row].add(contrib), jnp.zeros((), jnp.float32)

    result = lax.scan(add_row, jnp.zeros((cluster_groups, rank_dimension, columns), jnp.float32), (masked, coefficient_table, targets))
    dual_vector = result[0].astype(jnp.bfloat16)
    distant_part = jnp.einsum("qpo,qou->qpu", column_cluster_basis.reshape(cluster_groups, sample_points, rank_dimension).astype(jnp.float32), dual_vector.astype(jnp.float32), precision=lax.Precision.HIGHEST)
    from_above = jnp.roll(residual, 1, axis=0)
    from_below = jnp.roll(residual, -1, axis=0)
    side_offset = near_side[:, :, None, None]
    neighbour = jnp.where(side_offset == -1, from_above, jnp.where(side_offset == 1, from_below, jnp.zeros_like(residual)))

    def near_block(inputs):
        own_tile, own_res, side_tile, side_res = inputs
        own_part = jnp.dot(own_tile.T, own_res, preferred_element_type=jnp.float32)
        side_part = jnp.dot(side_tile.T, side_res, preferred_element_type=jnp.float32)
        return own_part + side_part

    near_part = lax.map(near_block, (self_tiles.reshape(cluster_groups, sample_points, sample_points), flattened_result, side_tiles.reshape(cluster_groups, sample_points, sample_points), neighbour.reshape(cluster_groups, sample_points, columns)))
    gradient = (near_part + distant_part).reshape(grid_rows, grid_cols, sample_points, columns)
    return gradient
```

```python
import functools

import jax
import jax.numpy as jnp
from jax import lax
from jax.experimental import pallas as pl
from jax.experimental.pallas import tpu as pltpu
from jax.sharding import PartitionSpec as P

MESH = pl.DeviceIdType.MESH
CORES = 2
LANES = 128
TILE = 256
NEAR_TILE = 512
FIRST = 3


def contract(a, b):
    return lax.dot_general(
        a, b, (((0,), (0,)), ((), ())), preferred_element_type=jnp.float32
    )


def pieces_of(leaf, blocks):
    quarter = leaf // 4
    pieces = [(c, r * quarter, quarter) for c in range(blocks) for r in range(4)]
    c, start, size = pieces.pop()
    return pieces + [(c, start, size // 2), (c, start + size // 2, size // 2)]


def kernel(
    rows, cols, pieces,
    near_hbm, count_hbm, tgt_hbm, rank_hbm, x_hbm, rb_hbm, cb_hbm, coup_hbm, self_hbm, side_hbm,
    out_ref,
    near_ref, count_ref, tgt_ref, rank_ref, xf, xc, rb_ref, cb_ref, coup_ref, self_v, side_v,
    above, below, table, flat, mbuf, dpart, dcore, mout, min_ref,
    load_sem, xc_sem, up_s, up_r, dn_s, dn_r, c_s, c_r, m_s, m_r, d_s, d_r, e_s, e_r,
):
    half_chips = rows // CORES // 2
    groups = cols * half_chips
    leaf, width = xf.shape
    blocks = width // LANES
    rank = rb_ref.shape[0]
    positions, slots = coup_ref.shape
    row, col = lax.axis_index("row"), lax.axis_index("col")
    core, chip = lax.rem(row, CORES), row // CORES
    mirror, pair = lax.rem(chip, 2), chip // 2
    group = col * half_chips + pair

    def at_group(g):
        return (((lax.rem(g, half_chips)) * 2 + mirror) * CORES + core, g // half_chips)

    after = (lax.rem(row + 1, rows), col)
    before = (lax.rem(row + rows - 1, rows), col)
    partner = (chip * CORES + (1 - core), col)
    opposite = ((pair * 2 + (1 - mirror)) * CORES + core, col)
    strides = []
    while groups >> (len(strides) + 1):
        strides.append(groups >> (len(strides) + 1))
    others = [at_group(group + h * (1 - 2 * lax.rem(group // h, 2))) for h in strides]

    loads = [
        pltpu.make_async_copy(
            x_hbm.at[:, pl.ds(c * LANES, LANES)], xc.at[c], xc_sem.at[c]
        )
        for c in range(blocks)
    ]
    names = (
        (rb_hbm, rb_ref), (x_hbm, xf), (coup_hbm, coup_ref), (tgt_hbm, tgt_ref),
        (rank_hbm, rank_ref), (count_hbm, count_ref), (near_hbm, near_ref),
        (self_hbm, self_v), (cb_hbm, cb_ref), (side_hbm, side_v),
    )
    rest = [
        pltpu.make_async_copy(src, dst, load_sem.at[i]) for i, (src, dst) in enumerate(names)
    ]
    for load in loads + rest:
        load.start()
    (
        load_rb, load_x, load_coup, load_tgt, load_rank, load_count, load_near,
        load_self, load_cb, load_side,
    ) = rest

    barrier = pltpu.get_barrier_semaphore()
    friends = [after, before, opposite] + others
    for friend in friends:
        pl.semaphore_signal(barrier, inc=1, device_id=friend, device_id_type=MESH)

    load_rb.wait()
    load_x.wait()
    table[0] = jnp.dot(rb_ref[...], xf[...], preferred_element_type=jnp.float32).astype(
        jnp.bfloat16
    )
    for load in loads:
        load.wait()

    pl.semaphore_wait(barrier, len(friends))

    def send(src, dst, s, r, to):
        return pltpu.make_async_remote_copy(
            src_ref=src, dst_ref=dst, send_sem=s, recv_sem=r, device_id=to, device_id_type=MESH
        )

    hops = []
    for i, (c, start, size) in enumerate(pieces):
        part = pl.ds(start, size)
        hops.append((
            send(xc.at[c, part], above.at[c, part], up_s.at[i], up_r.at[i], after),
            send(xc.at[c, part], below.at[c, part], dn_s.at[i], dn_r.at[i], before),
        ))

    def launch(some):
        for up, down in some:
            up.start()
            down.start()

    early = sum(1 for c, _, _ in pieces if c < FIRST)
    launch(hops[:early])

    for load in (load_coup, load_tgt, load_rank, load_count):
        load.wait()
    position = lax.broadcasted_iota(jnp.int32, (positions, slots), 0)
    slot = lax.broadcasted_iota(jnp.int32, (positions, slots), 1)
    ranks = rank_ref[...]
    keep = (
        (lax.div(position, rank) < ranks)
        & (lax.rem(position, rank) < ranks)
        & (slot < count_ref[...])
    )
    masked = jnp.where(keep, coup_ref[...].astype(jnp.float32), 0.0).astype(jnp.bfloat16)
    index = lax.broadcasted_iota(jnp.int32, (4 * groups, slots), 0)
    kind, member = lax.div(index, groups), lax.rem(index, groups)
    target = (
        (lax.rem(member, half_chips) * 2 + lax.rem(kind, 2)) * CORES + lax.div(kind, 2)
    ) * cols + lax.div(member, half_chips)
    onehot = (target == tgt_ref[...]).astype(jnp.float32).astype(jnp.bfloat16)
    sums = lax.dot_general(
        onehot, masked, (((1,), (1,)), ((), ())), preferred_element_type=jnp.float32
    )
    per = LANES // rank
    place = lax.broadcasted_iota(jnp.int32, (groups, LANES), 1) // rank
    for a in range(rank):
        base = a // per * LANES
        line = jnp.zeros((groups, LANES), jnp.float32)
        for q in range(4):
            value = sums[q * groups : (q + 1) * groups, base : base + LANES]
            shift = (q - a % per) % per * rank
            if shift:
                value = pltpu.roll(value, shift, 1)
            line = jnp.where(place == q, value, line)
        flat[a] = line
    for g in range(groups):
        mbuf[0, g] = flat[:, g, :].astype(jnp.bfloat16)

    tiles = leaf // TILE

    def own(m, carry):
        at = pl.ds(pl.multiple_of(m * TILE, TILE), TILE)
        out_ref[at, :] = contract(self_v[:, at], xf[...])
        return carry

    load_self.wait()
    steps = len(strides) + 1
    done = 0
    lax.fori_loop(0, 1, own, 0)
    done = 1
    for k, h in enumerate(strides):
        n = 1 << k
        theirs = group // (2 * h) * (2 * h) + (1 - lax.rem(group // h, 2)) * h
        coefs = send(
            table.at[pl.ds(0, n)], table.at[pl.ds(n, n)], c_s.at[k], c_r.at[k], others[k]
        )
        blocks_out = mbuf.at[pl.ds(0, n), pl.ds(theirs, h)]
        blocks_in = mbuf.at[pl.ds(n, n), pl.ds(theirs, h)]
        coupled = send(blocks_out, blocks_in, m_s.at[k], m_r.at[k], others[k])
        coefs.start()
        coupled.start()
        upto = 1 + (tiles - 1) * (k + 1) // steps
        lax.fori_loop(done, upto, own, 0)
        done = upto
        coefs.wait()
        coupled.wait()

    part = contract(
        mbuf[:, group].reshape(groups * rank, LANES), table[...].reshape(groups * rank, width)
    )
    dpart[...] = part.reshape(4, rank, width)
    lax.fori_loop(done, tiles, own, 0)
    swap = send(dpart.at[pl.ds(2 * (1 - core), 2)], dcore, d_s, d_r, partner)
    swap.start()
    load_near.wait()
    load_side.wait()
    from_above = jnp.where(near_ref[...] == -1, 1.0, 0.0).astype(jnp.float32)
    from_below = jnp.where(near_ref[...] == 1, 1.0, 0.0).astype(jnp.float32)

    def near(c, some):
        for i in some:
            hops[i][0].wait()
            hops[i][1].wait()
        start = pieces[some[0]][1]
        size = sum(pieces[i][2] for i in some)
        part = pl.ds(start, size)
        values = (
            above[c, part, :].astype(jnp.float32) * from_above
            + below[c, part, :].astype(jnp.float32) * from_below
        ).astype(jnp.bfloat16)
        lanes = pl.ds(c * LANES, LANES)

        def body(m, carry):
            at = pl.ds(pl.multiple_of(m * NEAR_TILE, NEAR_TILE), NEAR_TILE)
            out_ref[at, lanes] += contract(side_v[part, at], values)
            return carry

        lax.fori_loop(0, leaf // NEAR_TILE, body, 0)

    def members(c):
        return [i for i, p in enumerate(pieces) if p[0] == c]

    swap.wait()
    mout[...] = (dpart[2 * core + 1 - mirror] + dcore[1 - mirror]).astype(jnp.bfloat16)
    cross = send(mout, min_ref, e_s, e_r, opposite)
    cross.start()
    launch(hops[early:])
    for c in range(FIRST - 1):
        near(c, members(c))
    cross.wait()
    dual = (
        dpart[2 * core + mirror] + dcore[mirror] + min_ref[...].astype(jnp.float32)
    ).astype(jnp.bfloat16)

    def distant(m, carry):
        at = pl.ds(pl.multiple_of(m * TILE, TILE), TILE)
        out_ref[at, :] += contract(cb_ref[:, at], dual)
        return carry

    load_cb.wait()
    lax.fori_loop(0, tiles, distant, 0)
    for c in range(FIRST - 1, blocks - 1):
        near(c, members(c))
    for i in members(blocks - 1):
        near(blocks - 1, [i])


def on_device(
    rows, cols, residual, self_tiles, side_tiles, row_cluster_basis, column_cluster_basis,
    couplings, near_side, adm_targets, adm_ranks, adm_count,
):
    leaf, width = residual.shape[2:]
    slots, rank = couplings.shape[2:4]
    groups = cols * (rows // CORES // 2)
    blocks = width // LANES
    pieces = pieces_of(leaf, blocks)
    stages = groups.bit_length() - 1
    count = len(pieces)
    hbm = pl.BlockSpec(memory_space=pltpu.HBM)
    dma = pltpu.SemaphoreType.DMA
    bf16 = jnp.bfloat16
    gradient = pl.pallas_call(
        functools.partial(kernel, rows, cols, pieces),
        out_shape=pltpu.VMEM((leaf, width), jnp.float32),
        in_specs=[hbm] * 10,
        out_specs=pl.BlockSpec(memory_space=pltpu.VMEM),
        scratch_shapes=[
            pltpu.VMEM((1, 1), jnp.int32),
            pltpu.VMEM((1, 1), jnp.int32),
            pltpu.VMEM((1, slots), jnp.int32),
            pltpu.VMEM((1, slots), jnp.int32),
            pltpu.VMEM((leaf, width), bf16),
            pltpu.VMEM((blocks, leaf, LANES), bf16),
            pltpu.VMEM((rank, leaf), bf16),
            pltpu.VMEM((rank, leaf), bf16),
            pltpu.VMEM((rank * rank, slots), bf16),
            pltpu.VMEM((leaf, leaf), bf16),
            pltpu.VMEM((leaf, leaf), bf16),
            pltpu.VMEM((blocks, leaf, LANES), bf16),
            pltpu.VMEM((blocks, leaf, LANES), bf16),
            pltpu.VMEM((groups, rank, width), bf16),
            pltpu.VMEM((rank, groups, LANES), jnp.float32),
            pltpu.VMEM((groups, groups, rank, LANES), bf16),
            pltpu.VMEM((4, rank, width), jnp.float32),
            pltpu.VMEM((2, rank, width), jnp.float32),
            pltpu.VMEM((rank, width), bf16),
            pltpu.VMEM((rank, width), bf16),
            dma((10,)), dma((blocks,)),
            dma((count,)), dma((count,)), dma((count,)), dma((count,)),
            dma((stages,)), dma((stages,)), dma((stages,)), dma((stages,)),
            dma, dma, dma, dma,
        ],
        compiler_params=pltpu.CompilerParams(
            collective_id=0, has_side_effects=True, vmem_limit_bytes=58 * 1024 * 1024
        ),
    )(
        near_side, adm_count, adm_targets.reshape(1, slots), adm_ranks.reshape(1, slots),
        residual[0, 0], row_cluster_basis[0, 0].T, column_cluster_basis[0, 0].T,
        couplings.reshape(slots, rank * rank).T, self_tiles[0, 0], side_tiles[0, 0],
    )
    return gradient[None, None]


def solution(mesh):
    placed = (
        P("row", "col", None, None),
        P("row", "col", None, None),
        P("row", "col", None, None),
        P("row", "col", None, None),
        P("row", "col", None, None),
        P("row", "col", None, None, None),
        P("row", "col"),
        P("row", "col", None),
        P("row", "col", None),
        P("row", "col"),
    )
    return jax.shard_map(
        functools.partial(on_device, mesh.shape["row"], mesh.shape["col"]),
        mesh=mesh,
        in_specs=placed,
        out_specs=P("row", "col", None, None),
        check_vma=False,
    )
```

```python
import functools

import jax
import jax.numpy as jnp
from jax import lax
from jax.experimental import pallas as pl
from jax.experimental.pallas import tpu as pltpu
from jax.sharding import PartitionSpec as P

MESH = pl.DeviceIdType.MESH
CORES = 2
LANES = 128
TILE = 256
NEAR_TILE = 512
EARLY = 10


def contract(a, b):
    return lax.dot_general(
        a, b, (((0,), (0,)), ((), ())), preferred_element_type=jnp.float32
    )


def pieces_of(leaf, blocks):
    quarter = leaf // 4
    pieces = [(c, r * quarter, quarter) for c in range(blocks) for r in range(4)]
    c, start, size = pieces.pop()
    return pieces + [(c, start, size // 2), (c, start + size // 2, size // 2)]


def kernel(
    rows, cols, pieces,
    near_hbm, count_hbm, tgt_hbm, rank_hbm, x_hbm, rb_hbm, cb_hbm, coup_hbm, self_hbm, side_hbm,
    out_ref,
    near_ref, count_ref, tgt_ref, rank_ref, xf, xc, rb_ref, cb_ref, coup_ref, self_v, side_v,
    above, below, turned, table, flat, mbuf, dpart, dcore, mout, min_ref,
    load_sem, xc_sem, up_s, up_r, dn_s, dn_r, c_s, c_r, m_s, m_r, d_s, d_r, e_s, e_r, relay,
):
    half_chips = rows // CORES // 2
    groups = cols * half_chips
    leaf, width = xf.shape
    blocks = width // LANES
    rank = rb_ref.shape[0]
    positions, slots = coup_ref.shape
    row, col = lax.axis_index("row"), lax.axis_index("col")
    core, chip = lax.rem(row, CORES), row // CORES
    mirror, pair = lax.rem(chip, 2), chip // 2
    group = col * half_chips + pair

    def at_group(g):
        return (((lax.rem(g, half_chips)) * 2 + mirror) * CORES + core, g // half_chips)

    after = (lax.rem(row + 1, rows), col)
    before = (lax.rem(row + rows - 1, rows), col)
    partner = (chip * CORES + (1 - core), col)
    opposite = ((pair * 2 + (1 - mirror)) * CORES + core, col)
    strides = []
    while groups >> (len(strides) + 1):
        strides.append(groups >> (len(strides) + 1))
    others = [at_group(group + h * (1 - 2 * lax.rem(group // h, 2))) for h in strides]

    relayed = cols % 4 == 0
    quad = lax.rem(col, 4)
    middle = lax.rem((quad + 1) // 2, 2)
    between = (row, col + 3 - 2 * quad)
    friends = [after, before, opposite]
    friends += [d for d, h in zip(others, strides) if not (relayed and h == 2 * half_chips)]
    barrier = pltpu.get_barrier_semaphore()
    for friend in friends:
        pl.semaphore_signal(barrier, inc=1, device_id=friend, device_id_type=MESH)
    if relayed:

        @pl.when(middle == 1)
        def _():
            pl.semaphore_signal(barrier, inc=1, device_id=between, device_id_type=MESH)

    loads = [
        pltpu.make_async_copy(
            x_hbm.at[:, pl.ds(c * LANES, LANES)], xc.at[c], xc_sem.at[c]
        )
        for c in range(blocks)
    ]
    names = (
        (rb_hbm, rb_ref), (x_hbm, xf), (coup_hbm, coup_ref), (tgt_hbm, tgt_ref),
        (rank_hbm, rank_ref), (count_hbm, count_ref), (near_hbm, near_ref),
        (self_hbm, self_v), (cb_hbm, cb_ref), (side_hbm, side_v),
    )
    rest = [
        pltpu.make_async_copy(src, dst, load_sem.at[i]) for i, (src, dst) in enumerate(names)
    ]
    for load in loads + rest:
        load.start()
    (
        load_rb, load_x, load_coup, load_tgt, load_rank, load_count, load_near,
        load_self, load_cb, load_side,
    ) = rest

    load_rb.wait()
    load_x.wait()
    table[0] = jnp.dot(rb_ref[...], xf[...], preferred_element_type=jnp.float32).astype(
        jnp.bfloat16
    )
    for load in loads:
        load.wait()

    pl.semaphore_wait(barrier, len(friends) + middle if relayed else len(friends))

    def send(src, dst, s, r, to):
        return pltpu.make_async_remote_copy(
            src_ref=src, dst_ref=dst, send_sem=s, recv_sem=r, device_id=to, device_id_type=MESH
        )

    hops = []
    for i, (c, start, size) in enumerate(pieces):
        part = pl.ds(start, size)
        hops.append((
            send(xc.at[c, part], above.at[c, part], up_s.at[i], up_r.at[i], after),
            send(xc.at[c, part], below.at[c, part], dn_s.at[i], dn_r.at[i], before),
        ))

    def launch(some):
        for up, down in some:
            up.start()
            down.start()

    launch(hops[:EARLY])
    if relayed:

        @pl.when(middle == 1)
        def _():
            for to in (col - 1, col + 1):
                pl.semaphore_signal(relay, inc=1, device_id=(row, to), device_id_type=MESH)


    for load in (load_coup, load_tgt, load_rank, load_count):
        load.wait()
    position = lax.broadcasted_iota(jnp.int32, (positions, slots), 0)
    slot = lax.broadcasted_iota(jnp.int32, (positions, slots), 1)
    ranks = rank_ref[...]
    keep = (
        (lax.div(position, rank) < ranks)
        & (lax.rem(position, rank) < ranks)
        & (slot < count_ref[...])
    )
    masked = jnp.where(keep, coup_ref[...].astype(jnp.float32), 0.0).astype(jnp.bfloat16)
    index = lax.broadcasted_iota(jnp.int32, (4 * groups, slots), 0)
    kind, member = lax.div(index, groups), lax.rem(index, groups)
    target = (
        (lax.rem(member, half_chips) * 2 + lax.rem(kind, 2)) * CORES + lax.div(kind, 2)
    ) * cols + lax.div(member, half_chips)
    onehot = (target == tgt_ref[...]).astype(jnp.float32).astype(jnp.bfloat16)
    sums = lax.dot_general(
        onehot, masked, (((1,), (1,)), ((), ())), preferred_element_type=jnp.float32
    )
    per = LANES // rank
    place = lax.broadcasted_iota(jnp.int32, (groups, LANES), 1) // rank
    for a in range(rank):
        base = a // per * LANES
        line = jnp.zeros((groups, LANES), jnp.float32)
        for q in range(4):
            value = sums[q * groups : (q + 1) * groups, base : base + LANES]
            shift = (q - a % per) % per * rank
            if shift:
                value = pltpu.roll(value, shift, 1)
            line = jnp.where(place == q, value, line)
        flat[a] = line
    for g in range(groups):
        mbuf[0, g] = flat[:, g, :].astype(jnp.bfloat16)

    tiles = leaf // TILE

    def own(m, carry):
        at = pl.ds(pl.multiple_of(m * TILE, TILE), TILE)
        out_ref[at, :] = contract(self_v[:, at], xf[...])
        return carry

    load_self.wait()
    steps = len(strides) + 1
    done = 0
    lax.fori_loop(0, 1, own, 0)
    done = 1
    for k, h in enumerate(strides):
        n = 1 << k
        theirs = group // (2 * h) * (2 * h) + (1 - lax.rem(group // h, 2)) * h
        coefs = send(
            table.at[pl.ds(0, n)], table.at[pl.ds(n, n)], c_s.at[k], c_r.at[k], others[k]
        )
        blocks_out = mbuf.at[pl.ds(0, n), pl.ds(theirs, h)]
        blocks_in = mbuf.at[pl.ds(n, n), pl.ds(theirs, h)]
        coupled = send(blocks_out, blocks_in, m_s.at[k], m_r.at[k], others[k])
        if relayed and h == 2 * half_chips:
            pl.semaphore_wait(relay, 1)
        coefs.start()
        coupled.start()
        upto = 1 + (tiles - 1) * (k + 1) // steps
        lax.fori_loop(done, upto, own, 0)
        done = upto
        coefs.wait()
        coupled.wait()

    part = contract(
        mbuf[:, group].reshape(groups * rank, LANES), table[...].reshape(groups * rank, width)
    )
    dpart[...] = part.reshape(4, rank, width)
    lax.fori_loop(done, tiles, own, 0)
    swap = send(dpart.at[pl.ds(2 * (1 - core), 2)], dcore, d_s, d_r, partner)
    swap.start()
    load_near.wait()
    load_side.wait()
    from_above = jnp.where(near_ref[...] == -1, 1.0, 0.0).astype(jnp.float32)
    from_below = jnp.where(near_ref[...] == 1, 1.0, 0.0).astype(jnp.float32)

    def neighbour(c, some):
        for i in some:
            hops[i][0].wait()
            hops[i][1].wait()
        part = pl.ds(pieces[some[0]][1], sum(pieces[i][2] for i in some))
        values = (
            above[c, part, :].astype(jnp.float32) * from_above
            + below[c, part, :].astype(jnp.float32) * from_below
        ).astype(jnp.bfloat16)
        return part, values, pl.ds(c * LANES, LANES)

    def near(c, some):
        part, values, lanes = neighbour(c, some)

        def body(m, carry):
            at = pl.ds(pl.multiple_of(m * NEAR_TILE, NEAR_TILE), NEAR_TILE)
            out_ref[at, lanes] += contract(side_v[part, at], values)
            return carry

        lax.fori_loop(0, leaf // NEAR_TILE, body, 0)

    def members(c):
        return [i for i, p in enumerate(pieces) if p[0] == c]

    swap.wait()
    mout[...] = (dpart[2 * core + 1 - mirror] + dcore[1 - mirror]).astype(jnp.bfloat16)
    cross = send(mout, min_ref, e_s, e_r, opposite)
    cross.start()
    launch(hops[EARLY:])
    for c in range(blocks - 2):
        near(c, members(c))
    cross.wait()
    dual = (
        dpart[2 * core + mirror] + dcore[mirror] + min_ref[...].astype(jnp.float32)
    ).astype(jnp.bfloat16)

    def distant(m, carry):
        at = pl.ds(pl.multiple_of(m * TILE, TILE), TILE)
        out_ref[at, :] += contract(cb_ref[:, at], dual)
        return carry

    load_cb.wait()
    lax.fori_loop(0, tiles, distant, 0)
    for c in range(blocks - 2, blocks - 1):
        near(c, members(c))
    last = len(pieces) - 1
    final = pl.ds(pieces[last][1], pieces[last][2])

    def turn(m, carry):
        at = pl.ds(pl.multiple_of(m * TILE, TILE), TILE)
        turned[at, :] = side_v[final, at].T
        return carry

    lax.fori_loop(0, tiles, turn, 0)
    for i in members(blocks - 1)[:-1]:
        near(blocks - 1, [i])
    _, values, lanes = neighbour(blocks - 1, [last])
    for m in range(leaf // NEAR_TILE):
        at = pl.ds(m * NEAR_TILE, NEAR_TILE)
        out_ref[at, lanes] += jnp.dot(
            turned[at, :], values, preferred_element_type=jnp.float32
        )


def on_device(
    rows, cols, residual, self_tiles, side_tiles, row_cluster_basis, column_cluster_basis,
    couplings, near_side, adm_targets, adm_ranks, adm_count,
):
    leaf, width = residual.shape[2:]
    slots, rank = couplings.shape[2:4]
    groups = cols * (rows // CORES // 2)
    blocks = width // LANES
    pieces = pieces_of(leaf, blocks)
    stages = groups.bit_length() - 1
    count = len(pieces)
    hbm = pl.BlockSpec(memory_space=pltpu.HBM)
    dma = pltpu.SemaphoreType.DMA
    bf16 = jnp.bfloat16
    gradient = pl.pallas_call(
        functools.partial(kernel, rows, cols, pieces),
        out_shape=pltpu.VMEM((leaf, width), jnp.float32),
        in_specs=[hbm] * 10,
        out_specs=pl.BlockSpec(memory_space=pltpu.VMEM),
        scratch_shapes=[
            pltpu.VMEM((1, 1), jnp.int32),
            pltpu.VMEM((1, 1), jnp.int32),
            pltpu.VMEM((1, slots), jnp.int32),
            pltpu.VMEM((1, slots), jnp.int32),
            pltpu.VMEM((leaf, width), bf16),
            pltpu.VMEM((blocks, leaf, LANES), bf16),
            pltpu.VMEM((rank, leaf), bf16),
            pltpu.VMEM((rank, leaf), bf16),
            pltpu.VMEM((rank * rank, slots), bf16),
            pltpu.VMEM((leaf, leaf), bf16),
            pltpu.VMEM((leaf, leaf), bf16),
            pltpu.VMEM((blocks, leaf, LANES), bf16),
            pltpu.VMEM((blocks, leaf, LANES), bf16),
            pltpu.VMEM((leaf, pieces[-1][2]), bf16),
            pltpu.VMEM((groups, rank, width), bf16),
            pltpu.VMEM((rank, groups, LANES), jnp.float32),
            pltpu.VMEM((groups, groups, rank, LANES), bf16),
            pltpu.VMEM((4, rank, width), jnp.float32),
            pltpu.VMEM((2, rank, width), jnp.float32),
            pltpu.VMEM((rank, width), bf16),
            pltpu.VMEM((rank, width), bf16),
            dma((10,)), dma((blocks,)),
            dma((count,)), dma((count,)), dma((count,)), dma((count,)),
            dma((stages,)), dma((stages,)), dma((stages,)), dma((stages,)),
            dma, dma, dma, dma, pltpu.SemaphoreType.REGULAR,
        ],
        compiler_params=pltpu.CompilerParams(
            collective_id=0, has_side_effects=True, vmem_limit_bytes=58 * 1024 * 1024
        ),
    )(
        near_side, adm_count, adm_targets.reshape(1, slots), adm_ranks.reshape(1, slots),
        residual[0, 0], row_cluster_basis[0, 0].T, column_cluster_basis[0, 0].T,
        couplings.reshape(slots, rank * rank).T, self_tiles[0, 0], side_tiles[0, 0],
    )
    return gradient[None, None]


def solution(mesh):
    placed = (
        P("row", "col", None, None),
        P("row", "col", None, None),
        P("row", "col", None, None),
        P("row", "col", None, None),
        P("row", "col", None, None),
        P("row", "col", None, None, None),
        P("row", "col"),
        P("row", "col", None),
        P("row", "col", None),
        P("row", "col"),
    )
    return jax.shard_map(
        functools.partial(on_device, mesh.shape["row"], mesh.shape["col"]),
        mesh=mesh,
        in_specs=placed,
        out_specs=P("row", "col", None, None),
        check_vma=False,
    )
```

```python
import functools

import jax
import jax.numpy as jnp
from jax import lax
from jax.experimental import pallas as pl
from jax.experimental.pallas import tpu as pltpu
from jax.sharding import PartitionSpec as P

MESH = pl.DeviceIdType.MESH
CORES = 2
LANES = 128
TILE = 256
NEAR_TILE = 512
FINAL_STEPS = 4


def contract(a, b):
    return lax.dot_general(
        a, b, (((0,), (0,)), ((), ())), preferred_element_type=jnp.float32
    )


def pieces_of(leaf, blocks):
    half, quarter, eighth = leaf // 2, leaf // 4, leaf // 8
    pieces = [(c, 0, leaf) for c in range(blocks - 2)]
    c = blocks - 2
    lent = leaf // 8
    pieces += [(c, 0, half), (c, half, half - lent), (c, leaf - lent, lent)]
    c = blocks - 1
    pieces += [(c, 0, half), (c, half, quarter)]
    pieces += [(c, leaf - 2 * eighth, eighth), (c, leaf - eighth, eighth)]
    return pieces


def kernel(
    rows, cols, pieces,
    near_hbm, count_hbm, tgt_hbm, rank_hbm, x_hbm, rb_hbm, cb_hbm, coup_hbm, self_hbm, side_hbm,
    out_ref, turned, ending,
    near_ref, count_ref, tgt_ref, rank_ref, xf, xc, rb_ref, cb_ref, coup_ref, self_v, side_v,
    beside, table, flat, mbuf, dpart, dcore, mout, min_ref,
    load_sem, xc_sem, far_s, far_r, close_s, close_r, c_s, c_r, m_s, m_r, d_s, d_r, e_s, e_r, help_s, relay,
):
    half_chips = rows // CORES // 2
    groups = cols * half_chips
    leaf, width = xf.shape
    blocks = width // LANES
    rank = rb_ref.shape[0]
    positions, slots = coup_ref.shape
    row, col = lax.axis_index("row"), lax.axis_index("col")
    core, chip = lax.rem(row, CORES), row // CORES
    mirror, pair = lax.rem(chip, 2), chip // 2
    group = col * half_chips + pair

    def at_group(g):
        return (((lax.rem(g, half_chips)) * 2 + mirror) * CORES + core, g // half_chips)

    partner = (chip * CORES + (1 - core), col)
    away = (lax.rem(row + rows + 2 * core - 1, rows), col)
    partners_away = (lax.rem(chip * CORES + (1 - core) + rows + 1 - 2 * core, rows), col)
    opposite = ((pair * 2 + (1 - mirror)) * CORES + core, col)
    strides = []
    while groups >> (len(strides) + 1):
        strides.append(groups >> (len(strides) + 1))
    others = [at_group(group + h * (1 - 2 * lax.rem(group // h, 2))) for h in strides]

    relayed = cols % 4 == 0
    quad = lax.rem(col, 4)
    middle = lax.rem((quad + 1) // 2, 2)
    between = (row, col + 3 - 2 * quad)
    friends = [partner, away, opposite]
    friends += [d for d, h in zip(others, strides) if not (relayed and h == 2 * half_chips)]
    barrier = pltpu.get_barrier_semaphore()
    for friend in friends:
        pl.semaphore_signal(barrier, inc=1, device_id=friend, device_id_type=MESH)
    if relayed:

        @pl.when(middle == 1)
        def _():
            pl.semaphore_signal(barrier, inc=1, device_id=between, device_id_type=MESH)

    loads = [
        pltpu.make_async_copy(
            x_hbm.at[:, pl.ds(c * LANES, LANES)], xc.at[c], xc_sem.at[c]
        )
        for c in range(blocks)
    ]
    names = (
        (rb_hbm, rb_ref), (x_hbm, xf), (coup_hbm, coup_ref), (tgt_hbm, tgt_ref),
        (rank_hbm, rank_ref), (count_hbm, count_ref), (near_hbm, near_ref),
        (self_hbm, self_v), (cb_hbm, cb_ref), (side_hbm, side_v),
    )
    rest = [
        pltpu.make_async_copy(src, dst, load_sem.at[i]) for i, (src, dst) in enumerate(names)
    ]
    for load in loads + rest:
        load.start()
    (
        load_rb, load_x, load_coup, load_tgt, load_rank, load_count, load_near,
        load_self, load_cb, load_side,
    ) = rest

    load_rb.wait()
    load_x.wait()
    table[0] = jnp.dot(rb_ref[...], xf[...], preferred_element_type=jnp.float32).astype(
        jnp.bfloat16
    )
    for load in loads:
        load.wait()

    pl.semaphore_wait(barrier, len(friends) + middle if relayed else len(friends))

    def send(src, dst, s, r, to):
        return pltpu.make_async_remote_copy(
            src_ref=src, dst_ref=dst, send_sem=s, recv_sem=r, device_id=to, device_id_type=MESH
        )

    far, close = [], []
    for i, (c, start, size) in enumerate(pieces):
        part = pl.ds(start, size)
        far.append(
            send(xc.at[c, part], beside.at[1 - core, c, part], far_s.at[i], far_r.at[i], away)
        )
        close.append(
            send(xc.at[c, part], beside.at[core, c, part], close_s.at[i], close_r.at[i], partner)
        )
    early, last = blocks - 1, len(pieces) - 1
    lent = early + 1
    c, start, size = pieces[lent]
    part = pl.ds(start, size)
    helper = core == 1
    lends = chip != rows // CORES - 1
    relief = send(
        beside.at[1 - core, c, part], beside.at[core, c, part], help_s, far_r.at[lent],
        partners_away,
    )

    for copy in far[:early] + close:
        copy.start()
    if relayed:

        @pl.when(middle == 1)
        def _():
            for to in (col - 1, col + 1):
                pl.semaphore_signal(relay, inc=1, device_id=(row, to), device_id_type=MESH)


    for load in (load_coup, load_tgt, load_rank, load_count):
        load.wait()
    position = lax.broadcasted_iota(jnp.int32, (positions, slots), 0)
    slot = lax.broadcasted_iota(jnp.int32, (positions, slots), 1)
    ranks = rank_ref[...]
    keep = (
        (lax.div(position, rank) < ranks)
        & (lax.rem(position, rank) < ranks)
        & (slot < count_ref[...])
    )
    masked = jnp.where(keep, coup_ref[...].astype(jnp.float32), 0.0).astype(jnp.bfloat16)
    index = lax.broadcasted_iota(jnp.int32, (4 * groups, slots), 0)
    kind, member = lax.div(index, groups), lax.rem(index, groups)
    target = (
        (lax.rem(member, half_chips) * 2 + lax.rem(kind, 2)) * CORES + lax.div(kind, 2)
    ) * cols + lax.div(member, half_chips)
    onehot = (target == tgt_ref[...]).astype(jnp.float32).astype(jnp.bfloat16)
    sums = lax.dot_general(
        onehot, masked, (((1,), (1,)), ((), ())), preferred_element_type=jnp.float32
    )
    per = LANES // rank
    place = lax.broadcasted_iota(jnp.int32, (groups, LANES), 1) // rank
    for a in range(rank):
        base = a // per * LANES
        line = jnp.zeros((groups, LANES), jnp.float32)
        for q in range(4):
            value = sums[q * groups : (q + 1) * groups, base : base + LANES]
            shift = (q - a % per) % per * rank
            if shift:
                value = pltpu.roll(value, shift, 1)
            line = jnp.where(place == q, value, line)
        flat[a] = line
    for g in range(groups):
        mbuf[0, g] = flat[:, g, :].astype(jnp.bfloat16)

    tiles = leaf // TILE

    def own(m, carry):
        at = pl.ds(pl.multiple_of(m * TILE, TILE), TILE)
        out_ref[at, :] = contract(self_v[:, at], xf[...])
        return carry

    load_self.wait()
    steps = len(strides) + 1
    done = 0
    lax.fori_loop(0, 1, own, 0)
    done = 1
    for k, h in enumerate(strides):
        n = 1 << k
        theirs = group // (2 * h) * (2 * h) + (1 - lax.rem(group // h, 2)) * h
        coefs = send(
            table.at[pl.ds(0, n)], table.at[pl.ds(n, n)], c_s.at[k], c_r.at[k], others[k]
        )
        blocks_out = mbuf.at[pl.ds(0, n), pl.ds(theirs, h)]
        blocks_in = mbuf.at[pl.ds(n, n), pl.ds(theirs, h)]
        coupled = send(blocks_out, blocks_in, m_s.at[k], m_r.at[k], others[k])
        if relayed and h == 2 * half_chips:
            pl.semaphore_wait(relay, 1)
        coefs.start()
        coupled.start()
        upto = 1 + (tiles - 1) * (k + 1) // steps
        lax.fori_loop(done, upto, own, 0)
        done = upto
        coefs.wait()
        coupled.wait()

    part = contract(
        mbuf[:, group].reshape(groups * rank, LANES), table[...].reshape(groups * rank, width)
    )
    dpart[...] = part.reshape(4, rank, width)
    lax.fori_loop(done, tiles, own, 0)
    swap = send(dpart.at[pl.ds(2 * (1 - core), 2)], dcore, d_s, d_r, partner)
    swap.start()
    load_near.wait()
    load_side.wait()
    from_above = jnp.where(near_ref[...] == -1, 1.0, 0.0).astype(jnp.float32)
    from_below = jnp.where(near_ref[...] == 1, 1.0, 0.0).astype(jnp.float32)

    def neighbour(c, some):
        for i in some:
            far[i].wait_recv()
        part = pl.ds(pieces[some[0]][1], sum(pieces[i][2] for i in some))
        values = (
            beside[0, c, part, :].astype(jnp.float32) * from_above
            + beside[1, c, part, :].astype(jnp.float32) * from_below
        ).astype(jnp.bfloat16)
        return part, values, pl.ds(c * LANES, LANES)

    def near(c, some):
        part, values, lanes = neighbour(c, some)

        def body(m, carry):
            at = pl.ds(pl.multiple_of(m * NEAR_TILE, NEAR_TILE), NEAR_TILE)
            out_ref[at, lanes] += contract(side_v[part, at], values)
            return carry

        lax.fori_loop(0, leaf // NEAR_TILE, body, 0)

    def members(c):
        return [i for i, p in enumerate(pieces) if p[0] == c]

    swap.wait()
    mout[...] = (dpart[2 * core + 1 - mirror] + dcore[1 - mirror]).astype(jnp.bfloat16)
    cross = send(mout, min_ref, e_s, e_r, opposite)
    cross.start()
    for copy in close:
        copy.wait()
    for i in range(early, len(pieces)):
        if i == lent:

            @pl.when(helper & lends)
            def _():
                relief.start()

            @pl.when(helper | jnp.logical_not(lends))
            def _():
                far[lent].start()
        else:
            far[i].start()
    for c in range(blocks - 2):
        near(c, members(c))
    cross.wait()
    dual = (
        dpart[2 * core + mirror] + dcore[mirror] + min_ref[...].astype(jnp.float32)
    ).astype(jnp.bfloat16)

    def distant(m, carry):
        at = pl.ds(pl.multiple_of(m * TILE, TILE), TILE)
        out_ref[at, :] += contract(cb_ref[:, at], dual)
        return carry

    load_cb.wait()
    lax.fori_loop(0, tiles, distant, 0)
    for c in range(blocks - 2, blocks - 1):
        near(c, members(c))
    final = pl.ds(pieces[last][1], pieces[last][2])

    def turn(m, carry):
        at = pl.ds(pl.multiple_of(m * TILE, TILE), TILE)
        turned[at, :] = side_v[final, at].T
        return carry

    lax.fori_loop(0, tiles, turn, 0)
    for i in members(blocks - 1)[:-1]:
        near(blocks - 1, [i])
    _, values, _ = neighbour(blocks - 1, [last])
    ending[...] = values
    for i, copy in enumerate(far):
        if i != lent:
            copy.wait_send()

    @pl.when(helper & lends)
    def _():
        relief.wait_send()

    @pl.when(helper | jnp.logical_not(lends))
    def _():
        far[lent].wait_send()


def finish(acc_ref, turned_ref, ending_ref, out_ref, block, body_sem, block_sem):
    leaf, width = acc_ref.shape
    body = width - LANES
    step = leaf // FINAL_STEPS
    copies = []
    for m in range(FINAL_STEPS):
        at = pl.ds(m * step, step)
        copies.append(pltpu.make_async_copy(
            acc_ref.at[at, pl.ds(0, body)], out_ref.at[at, pl.ds(0, body)], body_sem.at[m]
        ))
        copies[-1].start()
    for m in range(FINAL_STEPS):
        at = pl.ds(m * step, step)
        block[at, :] = acc_ref[at, pl.ds(body, LANES)] + jnp.dot(
            turned_ref[at, :], ending_ref[...], preferred_element_type=jnp.float32
        )
        copies.append(pltpu.make_async_copy(
            block.at[at], out_ref.at[at, pl.ds(body, LANES)], block_sem.at[m]
        ))
        copies[-1].start()
    for copy in copies:
        copy.wait()


def on_device(
    rows, cols, residual, self_tiles, side_tiles, row_cluster_basis, column_cluster_basis,
    couplings, near_side, adm_targets, adm_ranks, adm_count,
):
    leaf, width = residual.shape[2:]
    slots, rank = couplings.shape[2:4]
    groups = cols * (rows // CORES // 2)
    blocks = width // LANES
    pieces = pieces_of(leaf, blocks)
    stages = groups.bit_length() - 1
    count = len(pieces)
    hbm = pl.BlockSpec(memory_space=pltpu.HBM)
    dma = pltpu.SemaphoreType.DMA
    bf16 = jnp.bfloat16
    vmem = pl.BlockSpec(memory_space=pltpu.VMEM)
    final = pieces[-1][2]
    acc, turned, ending = pl.pallas_call(
        functools.partial(kernel, rows, cols, pieces),
        out_shape=(
            pltpu.VMEM((leaf, width), jnp.float32),
            pltpu.VMEM((leaf, final), bf16),
            pltpu.VMEM((final, LANES), bf16),
        ),
        in_specs=[hbm] * 10,
        out_specs=(vmem, vmem, vmem),
        scratch_shapes=[
            pltpu.VMEM((1, 1), jnp.int32),
            pltpu.VMEM((1, 1), jnp.int32),
            pltpu.VMEM((1, slots), jnp.int32),
            pltpu.VMEM((1, slots), jnp.int32),
            pltpu.VMEM((leaf, width), bf16),
            pltpu.VMEM((blocks, leaf, LANES), bf16),
            pltpu.VMEM((rank, leaf), bf16),
            pltpu.VMEM((rank, leaf), bf16),
            pltpu.VMEM((rank * rank, slots), bf16),
            pltpu.VMEM((leaf, leaf), bf16),
            pltpu.VMEM((leaf, leaf), bf16),
            pltpu.VMEM((2, blocks, leaf, LANES), bf16),
            pltpu.VMEM((groups, rank, width), bf16),
            pltpu.VMEM((rank, groups, LANES), jnp.float32),
            pltpu.VMEM((groups, groups, rank, LANES), bf16),
            pltpu.VMEM((4, rank, width), jnp.float32),
            pltpu.VMEM((2, rank, width), jnp.float32),
            pltpu.VMEM((rank, width), bf16),
            pltpu.VMEM((rank, width), bf16),
            dma((10,)), dma((blocks,)),
            dma((count,)), dma((count,)), dma((count,)), dma((count,)),
            dma((stages,)), dma((stages,)), dma((stages,)), dma((stages,)),
            dma, dma, dma, dma, dma, pltpu.SemaphoreType.REGULAR,
        ],
        compiler_params=pltpu.CompilerParams(
            collective_id=0, has_side_effects=True, vmem_limit_bytes=54 * 1024 * 1024
        ),
    )(
        near_side, adm_count, adm_targets.reshape(1, slots), adm_ranks.reshape(1, slots),
        residual[0, 0], row_cluster_basis[0, 0].T, column_cluster_basis[0, 0].T,
        couplings.reshape(slots, rank * rank).T, self_tiles[0, 0], side_tiles[0, 0],
    )
    gradient = pl.pallas_call(
        finish,
        out_shape=jax.ShapeDtypeStruct((leaf, width), jnp.float32),
        in_specs=[vmem] * 3,
        out_specs=pl.BlockSpec(memory_space=pl.ANY),
        scratch_shapes=[
            pltpu.VMEM((leaf, LANES), jnp.float32), dma((FINAL_STEPS,)), dma((FINAL_STEPS,)),
        ],
        compiler_params=pltpu.CompilerParams(vmem_limit_bytes=16 * 1024 * 1024),
    )(acc, turned, ending)
    return gradient[None, None]


def solution(mesh):
    placed = (
        P("row", "col", None, None),
        P("row", "col", None, None),
        P("row", "col", None, None),
        P("row", "col", None, None),
        P("row", "col", None, None),
        P("row", "col", None, None, None),
        P("row", "col"),
        P("row", "col", None),
        P("row", "col", None),
        P("row", "col"),
    )
    return jax.shard_map(
        functools.partial(on_device, mesh.shape["row"], mesh.shape["col"]),
        mesh=mesh,
        in_specs=placed,
        out_specs=P("row", "col", None, None),
        check_vma=False,
    )
```

```python
import functools

import jax
import jax.numpy as jnp
from jax import lax
from jax.experimental import pallas as pl
from jax.experimental.pallas import tpu as pltpu
from jax.sharding import PartitionSpec as P

MESH = pl.DeviceIdType.MESH
CORES = 2
LANES = 128
TILE = 256
NEAR_TILE = 512
FINAL_STEPS = 4


def contract(a, b):
    return lax.dot_general(
        a, b, (((0,), (0,)), ((), ())), preferred_element_type=jnp.float32
    )


def pieces_of(leaf, blocks):
    half, quarter = leaf // 2, leaf // 4
    pieces = [(c, 0, leaf) for c in range(blocks - 2)]
    c = blocks - 2
    lent = leaf // 16
    pieces += [(c, 0, half), (c, half, half - lent), (c, leaf - lent, lent)]
    c = blocks - 1
    pieces += [(c, 0, half), (c, half, quarter), (c, leaf - quarter, quarter)]
    return pieces


def kernel(
    rows, cols, pieces,
    near_hbm, count_hbm, tgt_hbm, rank_hbm, x_hbm, rb_hbm, cb_hbm, coup_hbm, self_hbm, side_hbm,
    out_ref, turned, ending,
    near_ref, count_ref, tgt_ref, rank_ref, xf, xc, rb_ref, cb_ref, coup_ref, self_v, side_v,
    beside, table, flat, mbuf, dpart, dcore, mout, min_ref,
    load_sem, xc_sem, far_s, far_r, close_s, close_r, c_s, c_r, m_s, m_r, d_s, d_r, e_s, e_r, help_s, relay,
):
    half_chips = rows // CORES // 2
    groups = cols * half_chips
    leaf, width = xf.shape
    blocks = width // LANES
    rank = rb_ref.shape[0]
    positions, slots = coup_ref.shape
    row, col = lax.axis_index("row"), lax.axis_index("col")
    core, chip = lax.rem(row, CORES), row // CORES
    mirror, pair = lax.rem(chip, 2), chip // 2
    group = col * half_chips + pair

    def at_group(g):
        return (((lax.rem(g, half_chips)) * 2 + mirror) * CORES + core, g // half_chips)

    partner = (chip * CORES + (1 - core), col)
    away = (lax.rem(row + rows + 2 * core - 1, rows), col)
    partners_away = (lax.rem(chip * CORES + (1 - core) + rows + 1 - 2 * core, rows), col)
    opposite = ((pair * 2 + (1 - mirror)) * CORES + core, col)
    strides = []
    while groups >> (len(strides) + 1):
        strides.append(groups >> (len(strides) + 1))
    others = [at_group(group + h * (1 - 2 * lax.rem(group // h, 2))) for h in strides]

    relayed = cols % 4 == 0
    quad = lax.rem(col, 4)
    middle = lax.rem((quad + 1) // 2, 2)
    between = (row, col + 3 - 2 * quad)
    friends = [partner, away, opposite]
    friends += [d for d, h in zip(others, strides) if not (relayed and h == 2 * half_chips)]
    barrier = pltpu.get_barrier_semaphore()
    for friend in friends:
        pl.semaphore_signal(barrier, inc=1, device_id=friend, device_id_type=MESH)
    if relayed:

        @pl.when(middle == 1)
        def _():
            pl.semaphore_signal(barrier, inc=1, device_id=between, device_id_type=MESH)

    loads = [
        pltpu.make_async_copy(
            x_hbm.at[:, pl.ds(c * LANES, LANES)], xc.at[c], xc_sem.at[c]
        )
        for c in range(blocks)
    ]
    names = (
        (rb_hbm, rb_ref), (x_hbm, xf), (coup_hbm, coup_ref), (tgt_hbm, tgt_ref),
        (rank_hbm, rank_ref), (count_hbm, count_ref), (near_hbm, near_ref),
        (self_hbm, self_v), (cb_hbm, cb_ref), (side_hbm, side_v),
    )
    rest = [
        pltpu.make_async_copy(src, dst, load_sem.at[i]) for i, (src, dst) in enumerate(names)
    ]
    for load in loads + rest:
        load.start()
    (
        load_rb, load_x, load_coup, load_tgt, load_rank, load_count, load_near,
        load_self, load_cb, load_side,
    ) = rest

    load_rb.wait()
    load_x.wait()
    table[0] = jnp.dot(rb_ref[...], xf[...], preferred_element_type=jnp.float32).astype(
        jnp.bfloat16
    )
    for load in loads:
        load.wait()

    pl.semaphore_wait(barrier, len(friends) + middle if relayed else len(friends))

    def send(src, dst, s, r, to):
        return pltpu.make_async_remote_copy(
            src_ref=src, dst_ref=dst, send_sem=s, recv_sem=r, device_id=to, device_id_type=MESH
        )

    far, close = [], []
    for i, (c, start, size) in enumerate(pieces):
        part = pl.ds(start, size)
        far.append(
            send(xc.at[c, part], beside.at[1 - core, c, part], far_s.at[i], far_r.at[i], away)
        )
        close.append(
            send(xc.at[c, part], beside.at[core, c, part], close_s.at[i], close_r.at[i], partner)
        )
    early = blocks - 1
    lent = early + 1
    c, start, size = pieces[lent]
    part = pl.ds(start, size)
    helper = core == jnp.where(chip == rows // CORES - 1, 0, 1)
    relief = send(
        beside.at[1 - core, c, part], beside.at[core, c, part], help_s, far_r.at[lent],
        partners_away,
    )

    for copy in far[:early] + close:
        copy.start()
    if relayed:

        @pl.when(middle == 1)
        def _():
            for to in (col - 1, col + 1):
                pl.semaphore_signal(relay, inc=1, device_id=(row, to), device_id_type=MESH)


    for load in (load_coup, load_tgt, load_rank, load_count):
        load.wait()
    position = lax.broadcasted_iota(jnp.int32, (positions, slots), 0)
    slot = lax.broadcasted_iota(jnp.int32, (positions, slots), 1)
    ranks = rank_ref[...]
    keep = (
        (lax.div(position, rank) < ranks)
        & (lax.rem(position, rank) < ranks)
        & (slot < count_ref[...])
    )
    masked = jnp.where(keep, coup_ref[...].astype(jnp.float32), 0.0).astype(jnp.bfloat16)
    index = lax.broadcasted_iota(jnp.int32, (4 * groups, slots), 0)
    kind, member = lax.div(index, groups), lax.rem(index, groups)
    target = (
        (lax.rem(member, half_chips) * 2 + lax.rem(kind, 2)) * CORES + lax.div(kind, 2)
    ) * cols + lax.div(member, half_chips)
    onehot = (target == tgt_ref[...]).astype(jnp.float32).astype(jnp.bfloat16)
    sums = lax.dot_general(
        onehot, masked, (((1,), (1,)), ((), ())), preferred_element_type=jnp.float32
    )
    per = LANES // rank
    place = lax.broadcasted_iota(jnp.int32, (groups, LANES), 1) // rank
    for a in range(rank):
        base = a // per * LANES
        line = jnp.zeros((groups, LANES), jnp.float32)
        for q in range(4):
            value = sums[q * groups : (q + 1) * groups, base : base + LANES]
            shift = (q - a % per) % per * rank
            if shift:
                value = pltpu.roll(value, shift, 1)
            line = jnp.where(place == q, value, line)
        flat[a] = line
    for g in range(groups):
        mbuf[0, g] = flat[:, g, :].astype(jnp.bfloat16)

    tiles = leaf // TILE

    def own(m, carry):
        at = pl.ds(pl.multiple_of(m * TILE, TILE), TILE)
        out_ref[at, :] = contract(self_v[:, at], xf[...])
        return carry

    load_self.wait()
    steps = len(strides) + 1
    done = 0
    lax.fori_loop(0, 1, own, 0)
    done = 1
    for k, h in enumerate(strides):
        n = 1 << k
        theirs = group // (2 * h) * (2 * h) + (1 - lax.rem(group // h, 2)) * h
        coefs = send(
            table.at[pl.ds(0, n)], table.at[pl.ds(n, n)], c_s.at[k], c_r.at[k], others[k]
        )
        blocks_out = mbuf.at[pl.ds(0, n), pl.ds(theirs, h)]
        blocks_in = mbuf.at[pl.ds(n, n), pl.ds(theirs, h)]
        coupled = send(blocks_out, blocks_in, m_s.at[k], m_r.at[k], others[k])
        if relayed and h == 2 * half_chips:
            pl.semaphore_wait(relay, 1)
        coefs.start()
        coupled.start()
        upto = 1 + (tiles - 1) * (k + 1) // steps
        lax.fori_loop(done, upto, own, 0)
        done = upto
        coefs.wait()
        coupled.wait()

    part = contract(
        mbuf[:, group].reshape(groups * rank, LANES), table[...].reshape(groups * rank, width)
    )
    dpart[...] = part.reshape(4, rank, width)
    lax.fori_loop(done, tiles, own, 0)
    swap = send(dpart.at[pl.ds(2 * (1 - core), 2)], dcore, d_s, d_r, partner)
    swap.start()
    load_near.wait()
    load_side.wait()
    from_above = jnp.where(near_ref[...] == -1, 1.0, 0.0).astype(jnp.float32)
    from_below = jnp.where(near_ref[...] == 1, 1.0, 0.0).astype(jnp.float32)

    def neighbour(c, some):
        for i in some:
            far[i].wait_recv()
        part = pl.ds(pieces[some[0]][1], sum(pieces[i][2] for i in some))
        values = (
            beside[0, c, part, :].astype(jnp.float32) * from_above
            + beside[1, c, part, :].astype(jnp.float32) * from_below
        ).astype(jnp.bfloat16)
        return part, values, pl.ds(c * LANES, LANES)

    def near(c, some):
        part, values, lanes = neighbour(c, some)

        def body(m, carry):
            at = pl.ds(pl.multiple_of(m * NEAR_TILE, NEAR_TILE), NEAR_TILE)
            out_ref[at, lanes] += contract(side_v[part, at], values)
            return carry

        lax.fori_loop(0, leaf // NEAR_TILE, body, 0)

    def members(c):
        return [i for i, p in enumerate(pieces) if p[0] == c]

    swap.wait()
    mout[...] = (dpart[2 * core + 1 - mirror] + dcore[1 - mirror]).astype(jnp.bfloat16)
    cross = send(mout, min_ref, e_s, e_r, opposite)
    cross.start()
    for copy in close:
        copy.wait()
    for i in range(early, len(pieces)):
        if i == lent:

            @pl.when(helper)
            def _():
                relief.start()
                far[lent].start()
        else:
            far[i].start()
    for c in range(blocks - 2):
        near(c, members(c))
    cross.wait()
    dual = (
        dpart[2 * core + mirror] + dcore[mirror] + min_ref[...].astype(jnp.float32)
    ).astype(jnp.bfloat16)

    def distant(m, carry):
        at = pl.ds(pl.multiple_of(m * TILE, TILE), TILE)
        out_ref[at, :] += contract(cb_ref[:, at], dual)
        return carry

    load_cb.wait()
    lax.fori_loop(0, tiles, distant, 0)
    for c in range(blocks - 2, blocks - 1):
        near(c, members(c))
    closing = members(blocks - 1)[-1:]
    rows_left = sum(pieces[i][2] for i in closing)
    final = pl.ds(leaf - rows_left, rows_left)

    def turn(m, carry):
        at = pl.ds(pl.multiple_of(m * TILE, TILE), TILE)
        turned[at, :] = side_v[final, at].T
        return carry

    lax.fori_loop(0, tiles, turn, 0)
    for i in members(blocks - 1)[:-1]:
        near(blocks - 1, [i])
    _, values, _ = neighbour(blocks - 1, closing)
    ending[...] = values
    for i, copy in enumerate(far):
        if i != lent:
            copy.wait_send()

    @pl.when(helper)
    def _():
        relief.wait_send()
        far[lent].wait_send()


def finish(acc_ref, turned_ref, ending_ref, out_ref, block, body_sem, block_sem):
    leaf, width = acc_ref.shape
    body = width - LANES
    step = leaf // FINAL_STEPS
    copies = []
    for m in range(FINAL_STEPS):
        at = pl.ds(m * step, step)
        copies.append(pltpu.make_async_copy(
            acc_ref.at[at, pl.ds(0, body)], out_ref.at[at, pl.ds(0, body)], body_sem.at[m]
        ))
        copies[-1].start()
    for m in range(FINAL_STEPS):
        at = pl.ds(m * step, step)
        block[at, :] = acc_ref[at, pl.ds(body, LANES)] + jnp.dot(
            turned_ref[at, :], ending_ref[...], preferred_element_type=jnp.float32
        )
        copies.append(pltpu.make_async_copy(
            block.at[at], out_ref.at[at, pl.ds(body, LANES)], block_sem.at[m]
        ))
        copies[-1].start()
    for copy in copies:
        copy.wait()


def on_device(
    rows, cols, residual, self_tiles, side_tiles, row_cluster_basis, column_cluster_basis,
    couplings, near_side, adm_targets, adm_ranks, adm_count,
):
    leaf, width = residual.shape[2:]
    slots, rank = couplings.shape[2:4]
    groups = cols * (rows // CORES // 2)
    blocks = width // LANES
    pieces = pieces_of(leaf, blocks)
    stages = groups.bit_length() - 1
    count = len(pieces)
    hbm = pl.BlockSpec(memory_space=pltpu.HBM)
    dma = pltpu.SemaphoreType.DMA
    bf16 = jnp.bfloat16
    vmem = pl.BlockSpec(memory_space=pltpu.VMEM)
    final = sum(p[2] for p in pieces[-1:])
    acc, turned, ending = pl.pallas_call(
        functools.partial(kernel, rows, cols, pieces),
        out_shape=(
            pltpu.VMEM((leaf, width), jnp.float32),
            pltpu.VMEM((leaf, final), bf16),
            pltpu.VMEM((final, LANES), bf16),
        ),
        in_specs=[hbm] * 10,
        out_specs=(vmem, vmem, vmem),
        scratch_shapes=[
            pltpu.VMEM((1, 1), jnp.int32),
            pltpu.VMEM((1, 1), jnp.int32),
            pltpu.VMEM((1, slots), jnp.int32),
            pltpu.VMEM((1, slots), jnp.int32),
            pltpu.VMEM((leaf, width), bf16),
            pltpu.VMEM((blocks, leaf, LANES), bf16),
            pltpu.VMEM((rank, leaf), bf16),
            pltpu.VMEM((rank, leaf), bf16),
            pltpu.VMEM((rank * rank, slots), bf16),
            pltpu.VMEM((leaf, leaf), bf16),
            pltpu.VMEM((leaf, leaf), bf16),
            pltpu.VMEM((2, blocks, leaf, LANES), bf16),
            pltpu.VMEM((groups, rank, width), bf16),
            pltpu.VMEM((rank, groups, LANES), jnp.float32),
            pltpu.VMEM((groups, groups, rank, LANES), bf16),
            pltpu.VMEM((4, rank, width), jnp.float32),
            pltpu.VMEM((2, rank, width), jnp.float32),
            pltpu.VMEM((rank, width), bf16),
            pltpu.VMEM((rank, width), bf16),
            dma((10,)), dma((blocks,)),
            dma((count,)), dma((count,)), dma((count,)), dma((count,)),
            dma((stages,)), dma((stages,)), dma((stages,)), dma((stages,)),
            dma, dma, dma, dma, dma, pltpu.SemaphoreType.REGULAR,
        ],
        compiler_params=pltpu.CompilerParams(
            collective_id=0, has_side_effects=True, vmem_limit_bytes=54 * 1024 * 1024
        ),
    )(
        near_side, adm_count, adm_targets.reshape(1, slots), adm_ranks.reshape(1, slots),
        residual[0, 0], row_cluster_basis[0, 0].T, column_cluster_basis[0, 0].T,
        couplings.reshape(slots, rank * rank).T, self_tiles[0, 0], side_tiles[0, 0],
    )
    gradient = pl.pallas_call(
        finish,
        out_shape=jax.ShapeDtypeStruct((leaf, width), jnp.float32),
        in_specs=[vmem] * 3,
        out_specs=pl.BlockSpec(memory_space=pl.ANY),
        scratch_shapes=[
            pltpu.VMEM((leaf, LANES), jnp.float32), dma((FINAL_STEPS,)), dma((FINAL_STEPS,)),
        ],
        compiler_params=pltpu.CompilerParams(vmem_limit_bytes=16 * 1024 * 1024),
    )(acc, turned, ending)
    return gradient[None, None]


def solution(mesh):
    placed = (
        P("row", "col", None, None),
        P("row", "col", None, None),
        P("row", "col", None, None),
        P("row", "col", None, None),
        P("row", "col", None, None),
        P("row", "col", None, None, None),
        P("row", "col"),
        P("row", "col", None),
        P("row", "col", None),
        P("row", "col"),
    )
    return jax.shard_map(
        functools.partial(on_device, mesh.shape["row"], mesh.shape["col"]),
        mesh=mesh,
        in_specs=placed,
        out_specs=P("row", "col", None, None),
        check_vma=False,
    )
```

```python
import functools

import jax
import jax.numpy as jnp
from jax import lax
from jax.experimental import pallas as pl
from jax.experimental.pallas import tpu as pltpu
from jax.sharding import PartitionSpec as P

MESH = pl.DeviceIdType.MESH
CORES = 2
LANES = 128
TILE = 256
NEAR_TILE = 512
FINAL_STEPS = 4


def contract(a, b):
    return lax.dot_general(
        a, b, (((0,), (0,)), ((), ())), preferred_element_type=jnp.float32
    )


def pieces_of(leaf, blocks):
    half, quarter = leaf // 2, leaf // 4
    pieces = [(c, 0, leaf) for c in range(blocks - 2)]
    c = blocks - 2
    lent = leaf // 8 - leaf // 32
    pieces += [(c, 0, half), (c, half, half - lent), (c, leaf - lent, lent)]
    c = blocks - 1
    pieces += [(c, 0, half), (c, half, quarter), (c, leaf - quarter, quarter)]
    return pieces


def kernel(
    rows, cols, pieces,
    near_hbm, count_hbm, tgt_hbm, rank_hbm, x_hbm, rb_hbm, cb_hbm, coup_hbm, self_hbm, side_hbm,
    out_ref, turned, ending,
    near_ref, count_ref, tgt_ref, rank_ref, xf, xc, rb_ref, cb_ref, coup_ref, self_v, side_v,
    beside, table, flat, mbuf, dpart, dcore, mout, min_ref,
    load_sem, xc_sem, far_s, far_r, close_s, close_r, c_s, c_r, m_s, m_r, d_s, d_r, e_s, e_r, help_s, relay,
):
    half_chips = rows // CORES // 2
    groups = cols * half_chips
    leaf, width = xf.shape
    blocks = width // LANES
    rank = rb_ref.shape[0]
    positions, slots = coup_ref.shape
    row, col = lax.axis_index("row"), lax.axis_index("col")
    core, chip = lax.rem(row, CORES), row // CORES
    mirror, pair = lax.rem(chip, 2), chip // 2
    group = col * half_chips + pair

    def at_group(g):
        return (((lax.rem(g, half_chips)) * 2 + mirror) * CORES + core, g // half_chips)

    partner = (chip * CORES + (1 - core), col)
    away = (lax.rem(row + rows + 2 * core - 1, rows), col)
    partners_away = (lax.rem(chip * CORES + (1 - core) + rows + 1 - 2 * core, rows), col)
    opposite = ((pair * 2 + (1 - mirror)) * CORES + core, col)
    strides = []
    while groups >> (len(strides) + 1):
        strides.append(groups >> (len(strides) + 1))
    others = [at_group(group + h * (1 - 2 * lax.rem(group // h, 2))) for h in strides]

    relayed = cols % 4 == 0
    quad = lax.rem(col, 4)
    middle = lax.rem((quad + 1) // 2, 2)
    between = (row, col + 3 - 2 * quad)
    friends = [partner, away, opposite]
    friends += [d for d, h in zip(others, strides) if not (relayed and h == 2 * half_chips)]
    barrier = pltpu.get_barrier_semaphore()
    for friend in friends:
        pl.semaphore_signal(barrier, inc=1, device_id=friend, device_id_type=MESH)
    if relayed:

        @pl.when(middle == 1)
        def _():
            pl.semaphore_signal(barrier, inc=1, device_id=between, device_id_type=MESH)

    loads = [
        pltpu.make_async_copy(
            x_hbm.at[:, pl.ds(c * LANES, LANES)], xc.at[c], xc_sem.at[c]
        )
        for c in range(blocks)
    ]
    names = (
        (rb_hbm, rb_ref), (x_hbm, xf), (coup_hbm, coup_ref), (tgt_hbm, tgt_ref),
        (rank_hbm, rank_ref), (count_hbm, count_ref), (near_hbm, near_ref),
        (self_hbm, self_v), (cb_hbm, cb_ref), (side_hbm, side_v),
    )
    rest = [
        pltpu.make_async_copy(src, dst, load_sem.at[i]) for i, (src, dst) in enumerate(names)
    ]
    for load in loads + rest:
        load.start()
    (
        load_rb, load_x, load_coup, load_tgt, load_rank, load_count, load_near,
        load_self, load_cb, load_side,
    ) = rest

    load_rb.wait()
    load_x.wait()
    table[0] = jnp.dot(rb_ref[...], xf[...], preferred_element_type=jnp.float32).astype(
        jnp.bfloat16
    )
    for load in loads:
        load.wait()

    pl.semaphore_wait(barrier, len(friends) + middle if relayed else len(friends))

    def send(src, dst, s, r, to):
        return pltpu.make_async_remote_copy(
            src_ref=src, dst_ref=dst, send_sem=s, recv_sem=r, device_id=to, device_id_type=MESH
        )

    far, close = [], []
    for i, (c, start, size) in enumerate(pieces):
        part = pl.ds(start, size)
        far.append(
            send(xc.at[c, part], beside.at[1 - core, c, part], far_s.at[i], far_r.at[i], away)
        )
        close.append(
            send(xc.at[c, part], beside.at[core, c, part], close_s.at[i], close_r.at[i], partner)
        )
    early = blocks - 1
    lent = early + 1
    c, start, size = pieces[lent]
    part = pl.ds(start, size)
    helper = core == jnp.where(chip == rows // CORES - 1, 0, 1)
    relief = send(
        beside.at[1 - core, c, part], beside.at[core, c, part], help_s, far_r.at[lent],
        partners_away,
    )

    for copy in far[:early] + close:
        copy.start()
    if relayed:

        @pl.when(middle == 1)
        def _():
            for to in (col - 1, col + 1):
                pl.semaphore_signal(relay, inc=1, device_id=(row, to), device_id_type=MESH)


    for load in (load_coup, load_tgt, load_rank, load_count):
        load.wait()
    position = lax.broadcasted_iota(jnp.int32, (positions, slots), 0)
    slot = lax.broadcasted_iota(jnp.int32, (positions, slots), 1)
    ranks = rank_ref[...]
    keep = (
        (lax.div(position, rank) < ranks)
        & (lax.rem(position, rank) < ranks)
        & (slot < count_ref[...])
    )
    masked = jnp.where(keep, coup_ref[...].astype(jnp.float32), 0.0).astype(jnp.bfloat16)
    index = lax.broadcasted_iota(jnp.int32, (4 * groups, slots), 0)
    kind, member = lax.div(index, groups), lax.rem(index, groups)
    target = (
        (lax.rem(member, half_chips) * 2 + lax.rem(kind, 2)) * CORES + lax.div(kind, 2)
    ) * cols + lax.div(member, half_chips)
    onehot = (target == tgt_ref[...]).astype(jnp.float32).astype(jnp.bfloat16)
    sums = lax.dot_general(
        onehot, masked, (((1,), (1,)), ((), ())), preferred_element_type=jnp.float32
    )
    per = LANES // rank
    place = lax.broadcasted_iota(jnp.int32, (groups, LANES), 1) // rank
    for a in range(rank):
        base = a // per * LANES
        line = jnp.zeros((groups, LANES), jnp.float32)
        for q in range(4):
            value = sums[q * groups : (q + 1) * groups, base : base + LANES]
            shift = (q - a % per) % per * rank
            if shift:
                value = pltpu.roll(value, shift, 1)
            line = jnp.where(place == q, value, line)
        flat[a] = line
    for g in range(groups):
        mbuf[0, g] = flat[:, g, :].astype(jnp.bfloat16)

    tiles = leaf // TILE

    def own(m, carry):
        at = pl.ds(pl.multiple_of(m * TILE, TILE), TILE)
        out_ref[at, :] = contract(self_v[:, at], xf[...])
        return carry

    load_self.wait()
    steps = len(strides) + 1
    done = 0
    lax.fori_loop(0, 1, own, 0)
    done = 1
    for k, h in enumerate(strides):
        n = 1 << k
        theirs = group // (2 * h) * (2 * h) + (1 - lax.rem(group // h, 2)) * h
        coefs = send(
            table.at[pl.ds(0, n)], table.at[pl.ds(n, n)], c_s.at[k], c_r.at[k], others[k]
        )
        blocks_out = mbuf.at[pl.ds(0, n), pl.ds(theirs, h)]
        blocks_in = mbuf.at[pl.ds(n, n), pl.ds(theirs, h)]
        coupled = send(blocks_out, blocks_in, m_s.at[k], m_r.at[k], others[k])
        if relayed and h == 2 * half_chips:
            pl.semaphore_wait(relay, 1)
        coefs.start()
        coupled.start()
        upto = 1 + (tiles - 1) * (k + 1) // steps
        lax.fori_loop(done, upto, own, 0)
        done = upto
        coefs.wait()
        coupled.wait()

    part = contract(
        mbuf[:, group].reshape(groups * rank, LANES), table[...].reshape(groups * rank, width)
    )
    dpart[...] = part.reshape(4, rank, width)
    lax.fori_loop(done, tiles, own, 0)
    swap = send(dpart.at[pl.ds(2 * (1 - core), 2)], dcore, d_s, d_r, partner)
    swap.start()
    load_near.wait()
    load_side.wait()
    from_above = jnp.where(near_ref[...] == -1, 1.0, 0.0).astype(jnp.float32)
    from_below = jnp.where(near_ref[...] == 1, 1.0, 0.0).astype(jnp.float32)

    def neighbour(c, some):
        for i in some:
            far[i].wait_recv()
        part = pl.ds(pieces[some[0]][1], sum(pieces[i][2] for i in some))
        values = (
            beside[0, c, part, :].astype(jnp.float32) * from_above
            + beside[1, c, part, :].astype(jnp.float32) * from_below
        ).astype(jnp.bfloat16)
        return part, values, pl.ds(c * LANES, LANES)

    def near(c, some):
        part, values, lanes = neighbour(c, some)

        def body(m, carry):
            at = pl.ds(pl.multiple_of(m * NEAR_TILE, NEAR_TILE), NEAR_TILE)
            out_ref[at, lanes] += contract(side_v[part, at], values)
            return carry

        lax.fori_loop(0, leaf // NEAR_TILE, body, 0)

    def members(c):
        return [i for i, p in enumerate(pieces) if p[0] == c]

    swap.wait()
    mout[...] = (dpart[2 * core + 1 - mirror] + dcore[1 - mirror]).astype(jnp.bfloat16)
    cross = send(mout, min_ref, e_s, e_r, opposite)
    cross.start()
    for copy in close:
        copy.wait()
    for i in range(early, len(pieces)):
        if i == lent:

            @pl.when(helper)
            def _():
                relief.start()
                far[lent].start()
        else:
            far[i].start()
    for c in range(blocks - 2):
        near(c, members(c))
    cross.wait()
    dual = (
        dpart[2 * core + mirror] + dcore[mirror] + min_ref[...].astype(jnp.float32)
    ).astype(jnp.bfloat16)

    def distant(m, carry):
        at = pl.ds(pl.multiple_of(m * TILE, TILE), TILE)
        out_ref[at, :] += contract(cb_ref[:, at], dual)
        return carry

    load_cb.wait()
    lax.fori_loop(0, tiles, distant, 0)
    for c in range(blocks - 2, blocks - 1):
        near(c, members(c))
    closing = members(blocks - 1)[-1:]
    rows_left = sum(pieces[i][2] for i in closing)
    final = pl.ds(leaf - rows_left, rows_left)

    def turn(m, carry):
        at = pl.ds(pl.multiple_of(m * TILE, TILE), TILE)
        turned[at, :] = side_v[final, at].T
        return carry

    lax.fori_loop(0, tiles, turn, 0)
    for i in members(blocks - 1)[:-1]:
        near(blocks - 1, [i])
    _, values, _ = neighbour(blocks - 1, closing)
    ending[...] = values
    for i, copy in enumerate(far):
        if i != lent:
            copy.wait_send()

    @pl.when(helper)
    def _():
        relief.wait_send()
        far[lent].wait_send()


def finish(acc_ref, turned_ref, ending_ref, out_ref, block, body_sem, block_sem):
    leaf, width = acc_ref.shape
    body = width - LANES
    step = leaf // FINAL_STEPS
    copies = []
    for m in range(FINAL_STEPS):
        at = pl.ds(m * step, step)
        copies.append(pltpu.make_async_copy(
            acc_ref.at[at, pl.ds(0, body)], out_ref.at[at, pl.ds(0, body)], body_sem.at[m]
        ))
        copies[-1].start()
    for m in range(FINAL_STEPS):
        at = pl.ds(m * step, step)
        block[at, :] = acc_ref[at, pl.ds(body, LANES)] + jnp.dot(
            turned_ref[at, :], ending_ref[...], preferred_element_type=jnp.float32
        )
        copies.append(pltpu.make_async_copy(
            block.at[at], out_ref.at[at, pl.ds(body, LANES)], block_sem.at[m]
        ))
        copies[-1].start()
    for copy in copies:
        copy.wait()


def on_device(
    rows, cols, residual, self_tiles, side_tiles, row_cluster_basis, column_cluster_basis,
    couplings, near_side, adm_targets, adm_ranks, adm_count,
):
    leaf, width = residual.shape[2:]
    slots, rank = couplings.shape[2:4]
    groups = cols * (rows // CORES // 2)
    blocks = width // LANES
    pieces = pieces_of(leaf, blocks)
    stages = groups.bit_length() - 1
    count = len(pieces)
    hbm = pl.BlockSpec(memory_space=pltpu.HBM)
    dma = pltpu.SemaphoreType.DMA
    bf16 = jnp.bfloat16
    vmem = pl.BlockSpec(memory_space=pltpu.VMEM)
    final = sum(p[2] for p in pieces[-1:])
    acc, turned, ending = pl.pallas_call(
        functools.partial(kernel, rows, cols, pieces),
        out_shape=(
            pltpu.VMEM((leaf, width), jnp.float32),
            pltpu.VMEM((leaf, final), bf16),
            pltpu.VMEM((final, LANES), bf16),
        ),
        in_specs=[hbm] * 10,
        out_specs=(vmem, vmem, vmem),
        scratch_shapes=[
            pltpu.VMEM((1, 1), jnp.int32),
            pltpu.VMEM((1, 1), jnp.int32),
            pltpu.VMEM((1, slots), jnp.int32),
            pltpu.VMEM((1, slots), jnp.int32),
            pltpu.VMEM((leaf, width), bf16),
            pltpu.VMEM((blocks, leaf, LANES), bf16),
            pltpu.VMEM((rank, leaf), bf16),
            pltpu.VMEM((rank, leaf), bf16),
            pltpu.VMEM((rank * rank, slots), bf16),
            pltpu.VMEM((leaf, leaf), bf16),
            pltpu.VMEM((leaf, leaf), bf16),
            pltpu.VMEM((2, blocks, leaf, LANES), bf16),
            pltpu.VMEM((groups, rank, width), bf16),
            pltpu.VMEM((rank, groups, LANES), jnp.float32),
            pltpu.VMEM((groups, groups, rank, LANES), bf16),
            pltpu.VMEM((4, rank, width), jnp.float32),
            pltpu.VMEM((2, rank, width), jnp.float32),
            pltpu.VMEM((rank, width), bf16),
            pltpu.VMEM((rank, width), bf16),
            dma((10,)), dma((blocks,)),
            dma((count,)), dma((count,)), dma((count,)), dma((count,)),
            dma((stages,)), dma((stages,)), dma((stages,)), dma((stages,)),
            dma, dma, dma, dma, dma, pltpu.SemaphoreType.REGULAR,
        ],
        compiler_params=pltpu.CompilerParams(
            collective_id=0, has_side_effects=True, vmem_limit_bytes=54 * 1024 * 1024
        ),
    )(
        near_side, adm_count, adm_targets.reshape(1, slots), adm_ranks.reshape(1, slots),
        residual[0, 0], row_cluster_basis[0, 0].T, column_cluster_basis[0, 0].T,
        couplings.reshape(slots, rank * rank).T, self_tiles[0, 0], side_tiles[0, 0],
    )
    gradient = pl.pallas_call(
        finish,
        out_shape=jax.ShapeDtypeStruct((leaf, width), jnp.float32),
        in_specs=[vmem] * 3,
        out_specs=pl.BlockSpec(memory_space=pl.ANY),
        scratch_shapes=[
            pltpu.VMEM((leaf, LANES), jnp.float32), dma((FINAL_STEPS,)), dma((FINAL_STEPS,)),
        ],
        compiler_params=pltpu.CompilerParams(vmem_limit_bytes=16 * 1024 * 1024),
    )(acc, turned, ending)
    return gradient[None, None]


def solution(mesh):
    placed = (
        P("row", "col", None, None),
        P("row", "col", None, None),
        P("row", "col", None, None),
        P("row", "col", None, None),
        P("row", "col", None, None),
        P("row", "col", None, None, None),
        P("row", "col"),
        P("row", "col", None),
        P("row", "col", None),
        P("row", "col"),
    )
    return jax.shard_map(
        functools.partial(on_device, mesh.shape["row"], mesh.shape["col"]),
        mesh=mesh,
        in_specs=placed,
        out_specs=P("row", "col", None, None),
        check_vma=False,
    )
```
